32 devices in a mesh: rep: 2 (over x), dp: 16 (over y, z, core).
Axes of the slice: x: 2, y: 2, z: 4, core: 2. Of those that a mesh axis runs over, the one named last changes fastest.
Arguments:
- x: bfloat16 [32, 2048, 768], P(('rep', 'dp')), parts along dimension 0
- dy: bfloat16 [32, 2048, 768], P(('rep', 'dp')), parts along dimension 0
- w_gate: bfloat16 [2, 768, 2048], replicated
- w_up: bfloat16 [2, 768, 2048], replicated
- w_down: bfloat16 [2, 2048, 768], replicated
- m_w_gate: float32 [2, 768, 2048], P(None, 'dp')
- m_w_up: float32 [2, 768, 2048], P(None, 'dp')
- m_w_down: float32 [2, 2048, 768], P(None, 'dp')
- v_w_gate: float32 [2, 768, 2048], P(None, 'dp')
- v_w_up: float32 [2, 768, 2048], P(None, 'dp')
- v_w_down: float32 [2, 2048, 768], P(None, 'dp')
Outputs:
- output 1: bfloat16 [4, 768, 2048], P('rep'), parts along dimension 0
- output 2: bfloat16 [4, 768, 2048], P('rep'), parts along dimension 0
- output 3: bfloat16 [4, 2048, 768], P('rep'), parts along dimension 0
- output 4: float32 [4, 768, 2048], P('rep', 'dp'), parts along dimension 0
- output 5: float32 [4, 768, 2048], P('rep', 'dp'), parts along dimension 0
- output 6: float32 [4, 2048, 768], P('rep', 'dp'), parts along dimension 0
- output 7: float32 [4, 768, 2048], P('rep', 'dp'), parts along dimension 0
- output 8: float32 [4, 768, 2048], P('rep', 'dp'), parts along dimension 0
- output 9: float32 [4, 2048, 768], P('rep', 'dp'), parts along dimension 0
There are 2 independent parts. The reference program is written for one: setup_inputs(seed, part) draws one part's arguments, and reference() takes and returns one part's arrays. A program takes and returns all parts, laid end to end along the dimension named above; an argument that names none is the same for every part.
All inputs are finite; a program needn't handle non-finite values.
Results may differ from the reference program's by a relative error of at most 0.02.
Values are sent between devices in bfloat16 or wider.
A program may use at most 2 GiB of HBM per device.

```python
import jax
import jax.numpy as jnp
from jax import lax

SEQUENCES = 16
TOKENS = 2048
D = 768
FF = 2048
LAYERS = 2
NAMES = ("w_gate", "w_up", "w_down")
SHAPES = {"w_gate": (LAYERS, D, FF), "w_up": (LAYERS, D, FF), "w_down": (LAYERS, FF, D)}


def bump(key, n, height):
    away = (jnp.arange(n, dtype=jnp.int32) - jax.random.randint(key, (), 0, n, jnp.int32)) % n
    return jnp.where(away < n // 8, height, 1.0)


def together(key, own, strength):
    shared = jax.random.normal(key, own.shape[1:], jnp.float32)
    return (own + strength * shared) * lax.rsqrt(1 + strength * strength)


def setup_inputs(seed: int = 0, part: int = 0) -> dict:
    kx, kdy, ka, kb, kz, kf, kh, kl, *keys = jax.random.split(jax.random.key(seed), 8 + 3 * len(NAMES))
    kx, kdy, ka, kb = (jax.random.fold_in(k, part) for k in (kx, kdy, ka, kb))
    kw, km, kv = (keys[i::3] for i in range(3))
    shape = (SEQUENCES, TOKENS, D)
    much_x, much_dy = jax.random.uniform(kz, (2,), jnp.float32, 0.0, 1.0)
    loud = 2.0 ** jax.random.uniform(jax.random.fold_in(kz, 1), (), jnp.float32, -1.0, 2.0)
    layers = 2.0 ** jax.random.uniform(kl, (LAYERS, 1, 1), jnp.float32, -1.0, 1.0)
    x = together(ka, jax.random.normal(kx, shape, jnp.float32), much_x) * bump(kf, D, 4.0)
    dy = together(kb, jax.random.normal(kdy, shape, jnp.float32), much_dy)
    drawn = {"x": x.astype(jnp.bfloat16), "dy": (loud * dy * (SEQUENCES * TOKENS) ** -0.5).astype(jnp.bfloat16)}
    for key, name in zip(kw, NAMES, strict=True):
        w = jax.random.normal(key, SHAPES[name], jnp.float32) * SHAPES[name][1] ** -0.5
        drawn[name] = (w * {"w_gate": 1.0, "w_up": bump(kh, FF, 4.0), "w_down": layers}[name]).astype(jnp.bfloat16)
    for key, name in zip(km, NAMES, strict=True):
        drawn[f"m_{name}"] = 0.1 * jax.random.normal(key, SHAPES[name], jnp.float32)
    for key, name in zip(kv, NAMES, strict=True):
        drawn[f"v_{name}"] = jax.random.uniform(key, SHAPES[name], jnp.float32, 0.005, 0.015)
    return drawn


def matmul(a, w):
    return jnp.dot(a, w, preferred_element_type=jnp.float32).astype(jnp.bfloat16)


def normed(h):
    wide = h.astype(jnp.float32)
    scale = lax.rsqrt(jnp.mean(wide**2, -1, keepdims=True) + 1e-6)
    return (wide * scale).astype(jnp.bfloat16)


def layer(h, w):
    a = normed(h)
    gate = jnp.dot(a, w["w_gate"], preferred_element_type=jnp.float32)
    up = jnp.dot(a, w["w_up"], preferred_element_type=jnp.float32)
    return h + matmul((jax.nn.silu(gate) * up).astype(jnp.bfloat16), w["w_down"])


def adamw(w, m, v, g):
    m = 0.9 * m + 0.1 * g
    v = 0.95 * v + 0.05 * g * g
    step = m * lax.rsqrt(v + 1e-8) + 0.1 * w
    return (w - 0.02 * step).astype(jnp.bfloat16), m, v


def stack(weights, h):
    return lax.scan(lambda h, w: (layer(h, w), None), h, weights)[0]


def reference(x, dy, w_gate, w_up, w_down, m_w_gate, m_w_up, m_w_down, v_w_gate, v_w_up, v_w_down):
    weights = dict(zip(NAMES, (w_gate, w_up, w_down), strict=True))

    def take(so_far, sequence):
        h, by_y = sequence
        _, back = jax.vjp(lambda w: stack(w, h), weights)
        return jax.tree.map(lambda total, term: total + term.astype(jnp.float32), so_far, back(by_y)[0]), None

    none_yet = {name: jnp.zeros(w.shape, jnp.float32) for name, w in weights.items()}
    by_weights, _ = lax.scan(take, none_yet, (x, dy))
    gradients = [by_weights[name].astype(jnp.bfloat16).astype(jnp.float32) for name in NAMES]
    new = [
        adamw(w.astype(jnp.float32), m, v, g)
        for w, m, v, g in zip((w_gate, w_up, w_down), (m_w_gate, m_w_up, m_w_down), (v_w_gate, v_w_up, v_w_down), gradients, strict=True)
    ]
    return tuple(one[which] for which in range(3) for one in new)
```

```python
import functools

import jax
import jax.numpy as jnp
from jax import lax
from jax.experimental import pallas as pl
from jax.experimental.pallas import tpu as pltpu
from jax.sharding import PartitionSpec as P

F32, BF16 = jnp.float32, jnp.bfloat16
ANY = pl.BlockSpec(memory_space=pl.ANY)
TOK, D, FF = 2048, 768, 2048
LAYER = (1, 1, 1, 0, 0, 0)
KIND = (0, 1, 2, 0, 1, 2)


def dot(a, b, ca, cb):
    return lax.dot_general(a, b, (((ca,), (cb,)), ((), ())), preferred_element_type=F32)


def loop(lo, hi, f):
    def body(i, carry):
        f(i)
        return carry

    lax.fori_loop(lo, hi, body, 0)


def rows_of(i, size):
    return pl.ds(pl.multiple_of(i * size, size), size)


def norm(h):
    wide = h.astype(F32)
    return (wide * lax.rsqrt(jnp.mean(wide * wide, -1, keepdims=True) + 1e-6)).astype(BF16)


def kernel(
    x_hbm, dy_hbm, wg_hbm, wu_hbm, wd_hbm, mg, mu, md, vg, vu, vd,
    og, ou, od, omg, omu, omd, ovg, ovu, ovd, h1_hbm,
    hid, dgt, dup, abuf, ybuf, bd, bgu, rx1d, rx1gu, rx2d, rx2gu, rx3d, rx3gu, mvd, mvgu, wnd, wngu,
    lsem, hsem, mvsem, mvout, wout, s1, r1, s2, r2, s3, r3, s5, r5, s6, r6, s7, r7, free1, free2,
):
    me = lax.axis_index("dp")
    c = lax.rem(me, 2)
    z = lax.rem(me // 2, 4)
    y = me // 8

    def dev(y, z, c):
        return {"dp": (y * 4 + z) * 2 + c}

    core, across = dev(y, z, 1 - c), dev(1 - y, z, c)
    peers = [lax.rem(z + j, 4) for j in (1, 2, 3)]

    grads = (bd.at[1], bgu.at[0], bgu.at[1], bd.at[0], bgu.at[2], bgu.at[3])
    rx1 = (rx1d, rx1gu.at[0], rx1gu.at[1])
    rx2 = (rx2d, rx2gu.at[0], rx2gu.at[1])
    rx3 = (rx3d, rx3gu.at[0], rx3gu.at[1])
    mv = (mvd, mvgu.at[0], mvgu.at[1])
    wn = (wnd.at[0], wngu.at[0], wngu.at[1], wnd.at[1], wngu.at[2], wngu.at[3])
    out_w, out_m, out_v = (od, og, ou), (omd, omg, omu), (ovd, ovg, ovu)
    in_w, in_m, in_v = (wd_hbm, wg_hbm, wu_hbm), (md, mg, mu), (vd, vg, vu)

    def local(src, dst, sem):
        return pltpu.make_async_copy(src, dst, sem)

    def remote(src, dst, ssem, rsem, to):
        return pltpu.make_async_remote_copy(
            src_ref=src, dst_ref=dst, send_sem=ssem, recv_sem=rsem, device_id=to, device_id_type=pl.DeviceIdType.MESH
        )

    def signal(sem, to):
        pl.semaphore_signal(sem, inc=1, device_id=to, device_id_type=pl.DeviceIdType.MESH)

    def c1(k):
        return remote(grads[k].at[:, :, 1 - c], rx1[k % 3], s1.at[k], r1.at[k], core)

    def c2(k):
        return remote(grads[k].at[1 - y, :, c], rx2[k % 3], s2.at[k], r2.at[k], across)

    def c3(k, j):
        return remote(grads[k].at[y, peers[j], c], rx3[k % 3].at[j], s3.at[k, j], r3.at[k, j], dev(y, peers[j], c))

    def c5(k, j):
        dst = out_w[KIND[k]].at[LAYER[k], y, z, c]
        return remote(wn[k], dst, s5.at[k, j], r5.at[k, j], dev(y, peers[j], c))

    def c6(k):
        part = out_w[KIND[k]].at[LAYER[k], y, :, c]
        return remote(part, part, s6.at[k], r6.at[k], across)

    def c7(k):
        part = out_w[KIND[k]].at[LAYER[k], :, :, c]
        return remote(part, part, s7.at[k], r7.at[k], core)

    def mv_in(k):
        i, layer = k % 3, LAYER[k]
        return [
            local(in_m[i].at[layer], mv[i].at[0], mvsem.at[k, 0]),
            local(in_v[i].at[layer], mv[i].at[1], mvsem.at[k, 1]),
            local(in_w[i].at[layer, y, z, c], wn[k], mvsem.at[k, 2]),
        ]

    def mv_out(k):
        i, layer = k % 3, LAYER[k]
        return [
            local(mv[i].at[0], out_m[i].at[layer], mvout.at[k, 0]),
            local(mv[i].at[1], out_v[i].at[layer], mvout.at[k, 1]),
        ]

    def w_out(k):
        return local(wn[k], out_w[KIND[k]].at[LAYER[k], y, z, c], wout.at[k])

    def t1(k):
        if k >= 3:
            pl.semaphore_wait(free1.at[k % 3], 1)
        c1(k).start()

    def slabs(k):
        return grads[k].shape[-2] // 16

    def t2(k):
        g, a = grads[k], rx1[k % 3]
        c1(k).wait_recv()
        n = slabs(k)

        def add(i):
            zz, r = i // n, rows_of(lax.rem(i, n), 16)
            g[1 - y, zz, c, r, :] = (g[1 - y, zz, c, r, :].astype(F32) + a[1 - y, zz, r, :].astype(F32)).astype(BF16)

        loop(0, 4 * n, add)
        if k >= 3:
            pl.semaphore_wait(free2.at[k % 3], 1)
        c2(k).start()

    def t3(k):
        if k >= 3:
            for copy in mv_out(k - 3):
                copy.wait()
            for copy in mv_in(k):
                copy.start()
        g, a, b = grads[k], rx1[k % 3], rx2[k % 3]
        c2(k).wait_recv()
        n = slabs(k)
        for j in range(3):
            zz = peers[j]

            def add(i):
                r = rows_of(i, 16)
                total = g[y, zz, c, r, :].astype(F32) + a[y, zz, r, :].astype(F32) + b[zz, r, :].astype(F32)
                g[y, zz, c, r, :] = total.astype(BF16)

            loop(0, n, add)
            c3(k, j).start()

    def t4(k):
        g, a, b, d, s, w = grads[k], rx1[k % 3], rx2[k % 3], rx3[k % 3], mv[k % 3], wn[k]
        for copy in mv_in(k):
            copy.wait()
        for j in range(3):
            c3(k, j).wait_recv()

        def step(i):
            r = rows_of(i, 16)
            total = g[y, z, c, r, :].astype(F32) + a[y, z, r, :].astype(F32) + b[z, r, :].astype(F32)
            for j in range(3):
                total += d[j, r, :].astype(F32)
            grad = total.astype(BF16).astype(F32)
            m = 0.9 * s[0, r, :] + 0.1 * grad
            v = 0.95 * s[1, r, :] + 0.05 * grad * grad
            wide = w[r, :].astype(F32)
            s[0, r, :] = m
            s[1, r, :] = v
            w[r, :] = (wide - 0.02 * (m * lax.rsqrt(v + 1e-8) + 0.1 * wide)).astype(BF16)

        loop(0, slabs(k), step)
        for j in range(3):
            c5(k, j).start()
        w_out(k).start()
        for copy in mv_out(k):
            copy.start()
        if k < 3:
            signal(free1.at[k % 3], core)
            signal(free2.at[k % 3], across)

    def t5(k):
        w_out(k).wait()
        for j in range(3):
            c5(k, j).wait_recv()
        c6(k).start()

    def t6(k):
        c6(k).wait_recv()
        c7(k).start()

    def t7(k):
        c7(k).wait_recv()

    def wide_gu(buf, n):
        return buf[:, :, :, :, n].reshape(D, -1)

    def fwd(i):
        m, n = rows_of(i // 8, 1024), rows_of(lax.rem(i, 8), 256)
        am = abuf[m, :]
        gate, up = dot(am, wide_gu(bgu.at[0], n), 1, 0), dot(am, wide_gu(bgu.at[1], n), 1, 0)
        hid[m, n] = (gate * jax.nn.sigmoid(gate) * up).astype(BF16)

    def first(i):
        m = rows_of(i, 512)
        h = ybuf[m, :].astype(F32) + dot(hid[m, :], bd[0].reshape(FF, D), 1, 0).astype(BF16).astype(F32)
        h = h.astype(BF16)
        ybuf[m, :] = h
        abuf[m, :] = norm(h)

    def back(gi, ui, di, tm):
        def unit(i):
            m, n = rows_of(i // 8, tm), rows_of(lax.rem(i, 8), 256)
            b = lax.rem(i, 8)
            am = abuf[m, :]
            gate, up = dot(am, wide_gu(bgu.at[gi], n), 1, 0), dot(am, wide_gu(bgu.at[ui], n), 1, 0)
            wd = bd[di, b // 4, lax.rem(b, 4)].reshape(256, D)
            dh = dot(ybuf[m, :], wd, 1, 1).astype(BF16).astype(F32)
            s = jax.nn.sigmoid(gate)
            act = gate * s
            hid[m, n] = (act * up).astype(BF16)
            dup[m, n] = (dh * act).astype(BF16)
            dgt[m, n] = (dh * up * (s + act * (1.0 - s))).astype(BF16)

        return unit

    def grad_down(k):
        g = grads[k]

        def unit(i):
            n = rows_of(i, 512)
            out = dot(hid[:, n], ybuf[...], 0, 0).astype(BF16)
            g[i // 2, pl.ds(lax.rem(i, 2) * 2, 2)] = out.reshape(2, 2, 128, D)

        return unit

    def grad_gu(k, src):
        g = grads[k]

        def unit(i):
            n = rows_of(i, 512)
            g[:, :, :, :, n] = dot(abuf[...], src[:, n], 0, 0).astype(BF16).reshape(2, 4, 2, 48, 512)

        return unit

    def to_input(i):
        m = rows_of(i, 256)
        from_gate = dot(dgt[m, :], bgu[2].reshape(D, FF), 1, 1).astype(BF16).astype(F32)
        from_up = dot(dup[m, :], bgu[3].reshape(D, FF), 1, 1).astype(BF16).astype(F32)
        da = (from_gate + from_up).astype(BF16).astype(F32)
        h = hid[m, :D].astype(F32)
        scale = lax.rsqrt(jnp.mean(h * h, -1, keepdims=True) + 1e-6)
        dh = da * scale - h * (scale * scale * scale * jnp.mean(da * h, -1, keepdims=True))
        ybuf[m, :] = (ybuf[m, :].astype(F32) + dh.astype(BF16).astype(F32)).astype(BF16)

    def norm_rows(src, dst):
        def unit(i):
            m = rows_of(i, 256)
            dst[m, :] = norm(src[m, :])

        return unit

    load_x = local(x_hbm.at[0], ybuf, lsem.at[0])
    load_w0 = [local(wg_hbm.at[0], bgu.at[0], lsem.at[1]), local(wu_hbm.at[0], bgu.at[1], lsem.at[2]), local(wd_hbm.at[0], bd.at[0], lsem.at[3])]
    load_w1 = [local(wg_hbm.at[1], bgu.at[2], lsem.at[4]), local(wu_hbm.at[1], bgu.at[3], lsem.at[5]), local(wd_hbm.at[1], bd.at[1], lsem.at[6])]
    for copy in [load_x, *load_w0, *load_w1]:
        copy.start()
    barrier = pltpu.get_barrier_semaphore()
    for to in (core, across, *(dev(y, p, c) for p in peers)):
        signal(barrier, to)
    pl.semaphore_wait(barrier, 5)
    for k in range(3):
        for copy in mv_in(k):
            copy.start()

    load_x.wait()
    loop(0, 8, norm_rows(ybuf, abuf))
    load_w0[0].wait()
    load_w0[1].wait()
    loop(0, 16, fwd)
    load_w0[2].wait()
    loop(0, 4, first)
    save_h1 = local(ybuf, h1_hbm, hsem.at[0])
    save_h1.start()
    for copy in load_w1:
        copy.wait()
    save_h1.wait()
    load_dy = local(dy_hbm.at[0], ybuf, hsem.at[1])
    load_dy.start()
    load_dy.wait()
    loop(0, 32, back(2, 3, 1, 512))

    loop(0, 4, grad_down(0))
    t1(0)
    load_h1 = local(h1_hbm, hid.at[:, pl.ds(0, D)], hsem.at[2])
    load_h1.start()
    unit = grad_gu(1, dgt)
    loop(0, 2, unit)
    t2(0)
    loop(2, 4, unit)
    t1(1)
    unit = grad_gu(2, dup)
    loop(0, 2, unit)
    t2(1)
    loop(2, 4, unit)
    t1(2)
    load_x2 = local(x_hbm.at[0], abuf, hsem.at[3])
    load_x2.start()
    load_h1.wait()
    loop(0, 2, to_input)
    t2(2)
    loop(2, 4, to_input)
    t3(0)
    loop(4, 8, to_input)
    reload = [local(wg_hbm.at[0], bgu.at[2], hsem.at[4]), local(wu_hbm.at[0], bgu.at[3], hsem.at[5])]
    for copy in reload:
        copy.start()
    load_x2.wait()
    loop(0, 8, norm_rows(abuf, abuf))
    for copy in reload:
        copy.wait()
    unit = back(2, 3, 0, 512)
    loop(0, 8, unit)
    t3(1)
    loop(8, 16, unit)
    t4(0)
    loop(16, 32, unit)
    t3(2)

    unit = grad_down(3)
    loop(0, 2, unit)
    t4(1)
    loop(2, 4, unit)
    t1(3)
    unit = grad_gu(4, dgt)
    loop(0, 2, unit)
    t2(3)
    loop(2, 4, unit)
    t5(0)
    t1(4)
    unit = grad_gu(5, dup)
    loop(0, 2, unit)
    t2(4)
    loop(2, 4, unit)
    t4(2)
    t1(5)
    t5(1)
    t2(5)
    t6(0)
    t3(3)
    t5(2)
    t6(1)
    t3(4)
    t4(3)
    t6(2)
    t3(5)
    t5(3)
    t4(4)
    t6(3)
    t5(4)
    t4(5)
    t6(4)
    t5(5)
    t6(5)
    for k in range(6):
        t7(k)
        c1(k).wait_send()
        c2(k).wait_send()
        for j in range(3):
            c3(k, j).wait_send()
            c5(k, j).wait_send()
        c6(k).wait_send()
        c7(k).wait_send()
        if k >= 3:
            for copy in mv_out(k):
                copy.wait()


def solution(mesh):
    def step(x, dy, wg, wu, wd, mg, mu, md, vg, vu, vd):
        def split(w):
            return w.reshape(2, 2, 4, 2, -1, w.shape[-1])

        def shape(like, dtype):
            return jax.ShapeDtypeStruct(like.shape, dtype)

        wg6, wu6, wd6 = split(wg), split(wu), split(wd)
        vm = pltpu.VMEM
        dma = pltpu.SemaphoreType.DMA
        outs = pl.pallas_call(
            kernel,
            out_shape=[shape(wg6, BF16), shape(wu6, BF16), shape(wd6, BF16), *(shape(t, F32) for t in (mg, mu, md, vg, vu, vd)),
                       jax.ShapeDtypeStruct((TOK, D), BF16)],
            in_specs=[ANY] * 11,
            out_specs=[ANY] * 10,
            scratch_shapes=[
                vm((TOK, FF), BF16), vm((TOK, FF), BF16), vm((TOK, FF), BF16), vm((TOK, D), BF16), vm((TOK, D), BF16),
                vm((2, 2, 4, 2, 128, D), BF16), vm((4, 2, 4, 2, 48, FF), BF16),
                vm((2, 4, 128, D), BF16), vm((2, 2, 4, 48, FF), BF16),
                vm((4, 128, D), BF16), vm((2, 4, 48, FF), BF16),
                vm((3, 128, D), BF16), vm((2, 3, 48, FF), BF16),
                vm((2, 128, D), F32), vm((2, 2, 48, FF), F32),
                vm((2, 128, D), BF16), vm((4, 48, FF), BF16),
                dma((7,)), dma((6,)), dma((6, 3)), dma((6, 2)), dma((6,)),
                dma((6,)), dma((6,)), dma((6,)), dma((6,)), dma((6, 3)), dma((6, 3)), dma((6, 3)), dma((6, 3)),
                dma((6,)), dma((6,)), dma((6,)), dma((6,)),
                pltpu.SemaphoreType.REGULAR((3,)), pltpu.SemaphoreType.REGULAR((3,)),
            ],
            compiler_params=pltpu.CompilerParams(collective_id=0, has_side_effects=True, vmem_limit_bytes=67043328),
        )(x, dy, wg6, wu6, wd6, mg, mu, md, vg, vu, vd)
        new_w = [o.reshape(w.shape) for o, w in zip(outs[:3], (wg, wu, wd))]
        return (*new_w, *outs[3:9])

    rows = P(None, "dp", None)
    new_rows = P("rep", "dp", None)
    return jax.shard_map(
        step,
        mesh=mesh,
        in_specs=(P(("rep", "dp")), P(("rep", "dp")), P(), P(), P(), *([rows] * 6)),
        out_specs=(P("rep"), P("rep"), P("rep"), *([new_rows] * 6)),
        check_vma=False,
    )
```

```python
import functools

import jax
import jax.numpy as jnp
from jax import lax
from jax.experimental import pallas as pl
from jax.experimental.pallas import tpu as pltpu
from jax.sharding import PartitionSpec as P

F32, BF16 = jnp.float32, jnp.bfloat16
ANY = pl.BlockSpec(memory_space=pl.ANY)
TOK, D, FF = 2048, 768, 2048
PARTS = (2, 4, 4)
CHUNKS = tuple((layer, kind, part) for layer in (1, 0) for kind in range(3) for part in range(PARTS[kind]))
LAYER, KIND, PART = zip(*CHUNKS)
COUNT = len(CHUNKS)
HALF = COUNT // 2
BY_Y = tuple(way == "y" for way in "yyyyyyyyynyyyyyyynyn")
FROM_Z = tuple(way == "y" for way in "yyynyynyyynynyyynyyy")
BACK = 1024
ORDER = (
    (
        "", "", "", "", "", "c", "gc", "g", "", "", "c", "d", "gdh", "c", "h", "g", "cd", "e", "higec", "di", "g",
        "hc", "e", "f",
    ),
    (
        "ifdgj", "hcej", "if", "d",
    ),
    (
        "ahgb", "ejbiaf", "h", "d", "e", "", "bj", "i",
    ),
    (
        "f", "bad", "eh", "fj", "i", "m", "ambeq", "jfi", "q", "am", "", "nbj", "rfn", "qrma", "b", "j", "q", "omn",
        "osrqa", "s", "", "mnb", "r", "op",
    ),
    (
        "qpmt", "nto", "", "amq",
    ),
)
TAIL = ("lknsroltkpqsnropltsrklopsntklrspotsklpkt", "plktlk",)


def dot(a, b, ca, cb):
    return lax.dot_general(a, b, (((ca,), (cb,)), ((), ())), preferred_element_type=F32)


def loop(lo, hi, f):
    def body(i, carry):
        f(i)
        return carry

    lax.fori_loop(lo, hi, body, 0)


def rows_of(i, size):
    return pl.ds(pl.multiple_of(i * size, size), size)


def norm(h):
    wide = h.astype(F32)
    return (wide * lax.rsqrt(jnp.mean(wide * wide, -1, keepdims=True) + 1e-6)).astype(BF16)


def kernel(
    x_hbm, dy_hbm, wg_hbm, wu_hbm, wd_hbm, mg, mu, md, vg, vu, vd,
    og, ou, od, omg, omu, omd, ovg, ovu, ovd, h1_hbm,
    hid, dgt, dup, abuf, ybuf, bd, bgu, rx1d, rx1gu, rx2d, rx2gu, mvd, mvgu, wnd, wngu,
    lsem, hsem, mvsem, mvout, wout, s1, r1, s2, r2, sa, ra, sb, rb, s5, r5, s6, r6, s7, r7, s8, r8, s9, r9,
    free1, free2, free_a, free_b,
):
    me = lax.axis_index("dp")
    c = lax.rem(me, 2)
    z = lax.rem(me // 2, 4)
    y = me // 8

    def dev(y, z, c):
        return {"dp": (y * 4 + z) * 2 + c}

    core, across = dev(y, z, 1 - c), dev(1 - y, z, c)
    near = z + 1 - 2 * lax.rem(z, 2)
    far = 2 - 2 * (z // 2)
    inner_far = 2 - z // 2
    inner = jnp.logical_or(z == 1, z == 2)
    outer = jnp.logical_or(z == 0, z == 3)

    def cols(k):
        width = (D, FF, FF)[KIND[k]] // PARTS[KIND[k]]
        return pl.ds(PART[k] * width, width)

    def split(refs, dims):
        return tuple(
            ref.at[(*[slice(None)] * dims, cols(k))] for kind, ref in enumerate(refs) for k in range(HALF) if KIND[k] == kind
        )

    whole = (bd.at[1], bgu.at[0], bgu.at[1], bd.at[0], bgu.at[2], bgu.at[3])
    grads = split(whole[:3], 4) + split(whole[3:], 4)
    rx1 = split((rx1d, rx1gu.at[0], rx1gu.at[1]), 3)
    rx2 = split((rx2d, rx2gu.at[0], rx2gu.at[1]), 2)
    mv = split((mvd, mvgu.at[0], mvgu.at[1]), 2)
    wn = split((wnd.at[0], wngu.at[0], wngu.at[1]), 1) + split((wnd.at[1], wngu.at[2], wngu.at[3]), 1)
    out_w, out_m, out_v = (od, og, ou), (omd, omg, omu), (ovd, ovg, ovu)
    in_w, in_m, in_v = (wd_hbm, wg_hbm, wu_hbm), (md, mg, mu), (vd, vg, vu)

    def local(src, dst, sem):
        return pltpu.make_async_copy(src, dst, sem)

    def remote(src, dst, ssem, rsem, to):
        return pltpu.make_async_remote_copy(
            src_ref=src, dst_ref=dst, send_sem=ssem, recv_sem=rsem, device_id=to, device_id_type=pl.DeviceIdType.MESH
        )

    def signal(sem, to):
        pl.semaphore_signal(sem, inc=1, device_id=to, device_id_type=pl.DeviceIdType.MESH)

    def c1(k):
        return remote(grads[k].at[:, :, 1 - c], rx1[k % HALF], s1.at[k], r1.at[k], core)

    def c_y(k):
        if BY_Y[k]:
            return remote(grads[k].at[1 - y, :, c], rx2[k % HALF], s2.at[k], r2.at[k], across)
        return remote(grads[k].at[1 - y, z, c], rx2[k % HALF].at[0], s2.at[k], r2.at[k], across)

    def ys(k):
        return y if BY_Y[k] else slice(None)

    def c_near(k, count):
        which = pl.ds(jnp.where(z == 0, 1, 0), 3) if count == 3 else pl.ds(near, 1)
        g = grads[k]
        return remote(g.at[ys(k), which, c], g.at[ys(k), which, 1 - c], sa.at[k], ra.at[k], dev(y, near, c))

    def c_far(k, i):
        g = grads[k]
        dst = g.at[ys(k), far + 1 - i, 1 - c]
        return remote(g.at[ys(k), far + i, c], dst, sb.at[k, i], rb.at[k], dev(y, far + i, c))

    def place(k):
        return out_w[KIND[k]].at[LAYER[k], :, :, :, :, cols(k)]

    def c_near_w(k, p):
        there = place(k).at[y, z, c] if p == 0 else place(k).at[1 - y, z, c]
        return remote(wn[k] if p == 0 else there, there, s5.at[k, p], r5.at[k, p], dev(y, near, c))

    def c_far_w(k, p, slot=None):
        there = place(k).at[y, z, c] if p == 0 else place(k).at[1 - y, z, c]
        slot = lax.rem(z, 2) if slot is None else slot
        return remote(wn[k] if p == 0 else there, there, s6.at[k, p], r6.at[k, p, slot], dev(y, inner_far, c))

    def c_pass(k):
        part = place(k).at[y if FROM_Z[k] else slice(None), pl.ds(far, 2), c]
        return remote(part, part, s7.at[k], r7.at[k], dev(y, near, c))

    def c_y_w(k):
        if FROM_Z[k]:
            part = place(k).at[y, :, c]
            return remote(part, part, s8.at[k], r8.at[k], across)
        return remote(wn[k], place(k).at[y, z, c], s8.at[k], r8.at[k], across)

    def c_core_w(k):
        part = place(k).at[:, :, c]
        return remote(part, part, s9.at[k], r9.at[k], core)

    def mv_in(k):
        i, layer = KIND[k], LAYER[k]
        return [
            local(in_m[i].at[layer, :, cols(k)], mv[k % HALF].at[0], mvsem.at[k, 0]),
            local(in_v[i].at[layer, :, cols(k)], mv[k % HALF].at[1], mvsem.at[k, 1]),
            local(in_w[i].at[layer, y, z, c, :, cols(k)], wn[k], mvsem.at[k, 2]),
        ]

    def mv_out(k):
        i, layer = KIND[k], LAYER[k]
        return [
            local(mv[k % HALF].at[0], out_m[i].at[layer, :, cols(k)], mvout.at[k, 0]),
            local(mv[k % HALF].at[1], out_v[i].at[layer, :, cols(k)], mvout.at[k, 1]),
        ]

    def w_out(k):
        return local(wn[k], place(k).at[y, z, c], wout.at[k])

    def add_into(k, yy, zz, *more):
        g, a = grads[k], rx1[k % HALF]

        def add(i):
            r = rows_of(i, 16)
            total = g[yy, zz, c, r, :].astype(F32) + a[yy, zz, r, :].astype(F32)
            for ref, at in more:
                total += ref[(*at, r, slice(None))].astype(F32)
            g[yy, zz, c, r, :] = total.astype(BF16)

        loop(0, g.shape[-2] // 16, add)

    def send_core(k):
        if k >= HALF:
            pl.semaphore_wait(free1.at[k % HALF], 1)
        c1(k).start()

    def from_core(k):
        c1(k).wait_recv()
        c1(k).wait_send()
        signal(free_a.at[k], dev(y, near, c))
        signal(free_b.at[k], dev(y, inner_far, c))

    def send_near(k):
        both = (y,) if BY_Y[k] else (0, 1)
        more = [(rx2[k % HALF], None)] if BY_Y[k] else []

        def add(zz):
            for yy in both:
                add_into(k, yy, zz, *((ref, (zz,)) for ref, _ in more))

        pl.semaphore_wait(free_a.at[k], 1)

        @pl.when(outer)
        def _():
            first = jnp.where(z == 0, 1, 0)
            loop(0, 3, lambda i: add(first + i))
            c_near(k, 3).start()

        @pl.when(inner)
        def _():
            add(near)
            c_near(k, 1).start()

    def send_far(k):
        both = (y,) if BY_Y[k] else (0, 1)

        @pl.when(inner)
        def _():
            c_near(k, 3).wait_recv()
            pl.semaphore_wait(free_b.at[k], 2)
            for i in range(2):
                for yy in both:
                    more = [(grads[k], (yy, far + i, 1 - c))]
                    if BY_Y[k]:
                        more.append((rx2[k % HALF], (far + i,)))
                    add_into(k, yy, far + i, *more)
                c_far(k, i).start()

    def from_z(k):
        @pl.when(outer)
        def _():
            c_near(k, 1).wait_recv()

        c_far(k, 0).wait_recv()

    def prefetch(k):
        if k >= HALF:
            for copy in mv_out(k - HALF):
                copy.wait()
            for copy in mv_in(k):
                copy.start()

    def send_y(k):
        if k >= HALF:
            pl.semaphore_wait(free2.at[k % HALF], 1)
        if BY_Y[k]:
            loop(0, 4, lambda zz: add_into(k, 1 - y, zz))
        else:
            add_into(k, 1 - y, z, (grads[k], (1 - y, z, 1 - c)), (grads[k], (1 - y, near, 1 - c)))
        c_y(k).start()

    def update(k):
        g, a, b, s, w = grads[k], rx1[k % HALF], rx2[k % HALF], mv[k % HALF], wn[k]
        for copy in mv_in(k):
            copy.wait()
        kept = z if BY_Y[k] else 0

        def step(i):
            r = rows_of(i, 16)
            total = g[y, z, c, r, :].astype(F32) + a[y, z, r, :].astype(F32) + b[kept, r, :].astype(F32)
            total += g[y, z, 1 - c, r, :].astype(F32) + g[y, near, 1 - c, r, :].astype(F32)
            grad = total.astype(BF16).astype(F32)
            m = 0.9 * s[0, r, :] + 0.1 * grad
            v = 0.95 * s[1, r, :] + 0.05 * grad * grad
            wide = w[r, :].astype(F32)
            s[0, r, :] = m
            s[1, r, :] = v
            w[r, :] = (wide - 0.02 * (m * lax.rsqrt(v + 1e-8) + 0.1 * wide)).astype(BF16)

        loop(0, g.shape[-2] // 16, step)
        if not FROM_Z[k]:
            c_y_w(k).start()
        c_near_w(k, 0).start()
        c_far_w(k, 0).start()
        w_out(k).start()
        for copy in mv_out(k):
            copy.start()
        if k < HALF:
            signal(free1.at[k % HALF], core)
            signal(free2.at[k % HALF], across)

    def pass_on(k, parts):
        @pl.when(inner)
        def _():
            for p in range(parts):
                c_near_w(k, p).wait_recv()
                for slot in range(2):
                    c_far_w(k, p, slot).wait_recv()
            c_pass(k).start()

    def gathered_z(k, parts):
        @pl.when(outer)
        def _():
            for p in range(parts):
                c_near_w(k, p).wait_recv()
            c_pass(k).wait_recv()

    def steps(k):
        def second():
            from_core(k)
            send_y(k) if BY_Y[k] else send_near(k)

        def third():
            prefetch(k)
            if BY_Y[k]:
                c_y(k).wait_recv()
                send_near(k)
            else:
                send_far(k)

        def fourth():
            if BY_Y[k]:
                send_far(k)
            else:
                from_z(k)
                send_y(k)

        def fifth():
            if BY_Y[k]:
                from_z(k)
            else:
                c_y(k).wait_recv()
            update(k)

        def sixth():
            if FROM_Z[k]:
                pass_on(k, 1)
            else:
                c_y_w(k).wait_recv()
                c_near_w(k, 1).start()
                c_far_w(k, 1).start()

        def seventh():
            if FROM_Z[k]:
                w_out(k).wait()
                gathered_z(k, 1)
                c_y_w(k).start()
            else:
                pass_on(k, 2)

        def eighth():
            if FROM_Z[k]:
                c_y_w(k).wait_recv()
            else:
                w_out(k).wait()
                gathered_z(k, 2)
            c_core_w(k).start()

        return lambda: send_core(k), second, third, fourth, fifth, sixth, seventh, eighth

    def wide_gu(buf, n):
        return buf[:, :, :, :, n].reshape(D, -1)

    def fwd(i):
        m, n = rows_of(i // 8, 1024), rows_of(lax.rem(i, 8), 256)
        am = abuf[m, :]
        gate, up = dot(am, wide_gu(bgu.at[0], n), 1, 0), dot(am, wide_gu(bgu.at[1], n), 1, 0)
        hid[m, n] = (gate * jax.nn.sigmoid(gate) * up).astype(BF16)

    def first(i):
        m = rows_of(i, 512)
        h = ybuf[m, :].astype(F32) + dot(hid[m, :], bd[0].reshape(FF, D), 1, 0).astype(BF16).astype(F32)
        h = h.astype(BF16)
        ybuf[m, :] = h
        abuf[m, :] = norm(h)

    def back(gi, ui, di, tm):
        def unit(i):
            b = i // (TOK // tm)
            m, n = rows_of(lax.rem(i, TOK // tm), tm), rows_of(b, 256)
            am = abuf[m, :]
            gate, up = dot(am, wide_gu(bgu.at[gi], n), 1, 0), dot(am, wide_gu(bgu.at[ui], n), 1, 0)
            wd = bd[di, b // 4, lax.rem(b, 4)].reshape(256, D)
            dh = dot(ybuf[m, :], wd, 1, 1).astype(BF16).astype(F32)
            s = jax.nn.sigmoid(gate)
            act = gate * s
            hid[m, n] = (act * up).astype(BF16)
            dup[m, n] = (dh * act).astype(BF16)
            dgt[m, n] = (dh * up * (s + act * (1.0 - s))).astype(BF16)

        return unit

    def grad_down(k):
        g = whole[k]

        def unit(i):
            n = rows_of(i, 512)
            out = dot(hid[:, n], ybuf[...], 0, 0).astype(BF16)
            g[i // 2, pl.ds(lax.rem(i, 2) * 2, 2)] = out.reshape(2, 2, 128, D)

        return unit

    def grad_gu(k, src):
        g = whole[k]

        def unit(i):
            n = rows_of(i, 512)
            g[:, :, :, :, n] = dot(abuf[...], src[:, n], 0, 0).astype(BF16).reshape(2, 4, 2, 48, 512)

        return unit

    def to_input(i):
        m = rows_of(i, 256)
        from_gate = dot(dgt[m, :], bgu[2].reshape(D, FF), 1, 1).astype(BF16).astype(F32)
        from_up = dot(dup[m, :], bgu[3].reshape(D, FF), 1, 1).astype(BF16).astype(F32)
        da = (from_gate + from_up).astype(BF16).astype(F32)
        h = hid[m, :D].astype(F32)
        scale = lax.rsqrt(jnp.mean(h * h, -1, keepdims=True) + 1e-6)
        dh = da * scale - h * (scale * scale * scale * jnp.mean(da * h, -1, keepdims=True))
        ybuf[m, :] = (ybuf[m, :].astype(F32) + dh.astype(BF16).astype(F32)).astype(BF16)

    def norm_rows(src, dst):
        def unit(i):
            m = rows_of(i, 256)
            dst[m, :] = norm(src[m, :])

        return unit

    load_x = local(x_hbm.at[0], ybuf, lsem.at[0])
    load_w0 = [local(wg_hbm.at[0], bgu.at[0], lsem.at[1]), local(wu_hbm.at[0], bgu.at[1], lsem.at[2]), local(wd_hbm.at[0], bd.at[0], lsem.at[3])]
    load_w1 = [local(wg_hbm.at[1], bgu.at[2], lsem.at[4]), local(wu_hbm.at[1], bgu.at[3], lsem.at[5]), local(wd_hbm.at[1], bd.at[1], lsem.at[6])]
    for copy in [load_x, *load_w0, *load_w1]:
        copy.start()
    barrier = pltpu.get_barrier_semaphore()
    for to in (core, across, *(dev(y, lax.rem(z + j, 4), c) for j in (1, 2, 3))):
        signal(barrier, to)
    pl.semaphore_wait(barrier, 5)
    for k in range(HALF):
        for copy in mv_in(k):
            copy.start()

    load_x.wait()
    loop(0, 8, norm_rows(ybuf, abuf))
    load_w0[0].wait()
    load_w0[1].wait()
    loop(0, 16, fwd)
    load_w0[2].wait()
    loop(0, 4, first)
    save_h1 = local(ybuf, h1_hbm, hsem.at[0])
    save_h1.start()
    for copy in load_w1:
        copy.wait()
    save_h1.wait()
    load_dy = local(dy_hbm.at[0], ybuf, hsem.at[1])
    load_dy.start()
    load_dy.wait()

    load_h1 = local(h1_hbm, hid.at[:, pl.ds(0, D)], hsem.at[2])
    load_x2 = local(x_hbm.at[0], abuf, hsem.at[3])
    reload = [local(wg_hbm.at[0], bgu.at[2], hsem.at[4]), local(wu_hbm.at[0], bgu.at[3], hsem.at[5])]

    def before_input():
        load_x2.start()
        load_h1.start()
        load_h1.wait()

    def before_back():
        for copy in reload:
            copy.start()
        load_x2.wait()
        loop(0, 8, norm_rows(abuf, abuf))
        for copy in reload:
            copy.wait()

    left = [list(steps(k)) for k in range(COUNT)]

    def listed(letters):
        return [left[ord(letter) - ord("a")].pop(0) for letter in letters]

    plan = [[listed(letters) for letters in product] for product in ORDER]
    rest = listed("".join(TAIL))
    assert not any(left)

    def run(todo):
        for step in todo:
            step()

    def between(product, i, which):
        for at in which:
            if at and plan[product][at]:
                pl.when(i == at)(functools.partial(run, plan[product][at]))

    def plain(product, unit):
        def piece(i):
            between(product, i, range(len(ORDER[product])))
            unit(i)

        loop(0, len(ORDER[product]), piece)

    def by_quarters(product, unit, gate, up):
        each = len(ORDER[product]) // 4

        def quarter(q):
            def piece(j):
                between(product, q * each + j, [at for at in range(4 * each) if at % each < each - 2])
                unit(q * (each - 2) + j)

            loop(0, each - 2, piece)
            for last, grad in ((2, gate), (1, up)):
                for at in range(each - last, 4 * each, each):
                    if plan[product][at]:
                        pl.when(q == at // each)(functools.partial(run, plan[product][at]))
                grad(q)

        loop(0, 4, quarter)

    run(plan[0][0])
    by_quarters(0, back(2, 3, 1, BACK), grad_gu(1, dgt), grad_gu(2, dup))
    run(plan[1][0])
    plain(1, grad_down(0))
    run(plan[2][0])
    before_input()
    plain(2, to_input)
    run(plan[3][0])
    before_back()
    by_quarters(3, back(2, 3, 0, BACK), grad_gu(4, dgt), grad_gu(5, dup))
    run(plan[4][0])
    plain(4, grad_down(3))
    run(rest)

    for k in range(COUNT):
        c_core_w(k).wait_recv()
        c_y(k).wait_send()
        c_near_w(k, 0).wait_send()
        c_far_w(k, 0).wait_send()
        if not FROM_Z[k]:
            c_near_w(k, 1).wait_send()
            c_far_w(k, 1).wait_send()
        c_y_w(k).wait_send()
        c_core_w(k).wait_send()
        if k >= HALF:
            for copy in mv_out(k):
                copy.wait()

    @pl.when(outer)
    def _():
        for k in range(COUNT):
            c_near(k, 3).wait_send()

    @pl.when(inner)
    def _():
        for k in range(COUNT):
            c_near(k, 1).wait_send()
            c_pass(k).wait_send()
            for i in range(2):
                c_far(k, i).wait_send()


def solution(mesh):
    def step(x, dy, wg, wu, wd, mg, mu, md, vg, vu, vd):
        def split(w):
            return w.reshape(2, 2, 4, 2, -1, w.shape[-1])

        def shape(like, dtype):
            return jax.ShapeDtypeStruct(like.shape, dtype)

        wg6, wu6, wd6 = split(wg), split(wu), split(wd)
        vm = pltpu.VMEM
        dma = pltpu.SemaphoreType.DMA
        outs = pl.pallas_call(
            kernel,
            out_shape=[shape(wg6, BF16), shape(wu6, BF16), shape(wd6, BF16), *(shape(t, F32) for t in (mg, mu, md, vg, vu, vd)),
                       jax.ShapeDtypeStruct((TOK, D), BF16)],
            in_specs=[ANY] * 11,
            out_specs=[ANY] * 10,
            scratch_shapes=[
                vm((TOK, FF), BF16), vm((TOK, FF), BF16), vm((TOK, FF), BF16), vm((TOK, D), BF16), vm((TOK, D), BF16),
                vm((2, 2, 4, 2, 128, D), BF16), vm((4, 2, 4, 2, 48, FF), BF16),
                vm((2, 4, 128, D), BF16), vm((2, 2, 4, 48, FF), BF16),
                vm((4, 128, D), BF16), vm((2, 4, 48, FF), BF16),
                vm((2, 128, D), F32), vm((2, 2, 48, FF), F32),
                vm((2, 128, D), BF16), vm((4, 48, FF), BF16),
                dma((7,)), dma((6,)), dma((COUNT, 3)), dma((COUNT, 2)), dma((COUNT,)),
                *([dma((COUNT,))] * 6), dma((COUNT, 2)), dma((COUNT,)),
                dma((COUNT, 2)), dma((COUNT, 2)), dma((COUNT, 2)), dma((COUNT, 2, 2)), *([dma((COUNT,))] * 6),
                *(pltpu.SemaphoreType.REGULAR((n,)) for n in (HALF, HALF, COUNT, COUNT)),
            ],
            compiler_params=pltpu.CompilerParams(collective_id=0, has_side_effects=True, vmem_limit_bytes=67043328),
        )(x, dy, wg6, wu6, wd6, mg, mu, md, vg, vu, vd)
        new_w = [o.reshape(w.shape) for o, w in zip(outs[:3], (wg, wu, wd))]
        return (*new_w, *outs[3:9])

    rows = P(None, "dp", None)
    new_rows = P("rep", "dp", None)
    return jax.shard_map(
        step,
        mesh=mesh,
        in_specs=(P(("rep", "dp")), P(("rep", "dp")), P(), P(), P(), *([rows] * 6)),
        out_specs=(P("rep"), P("rep"), P("rep"), *([new_rows] * 6)),
        check_vma=False,
    )
```
